32 devices in a mesh: pool: 2 (over core), dev: 16 (over z, y, x).
Axes of the slice: x: 2, y: 2, z: 4, core: 2. Of those that a mesh axis runs over, the one named last changes fastest.
Arguments:
- hidden: bfloat16 [256, 7168], P('dev'), may hold values from -240 to 240
- ffn_gain: float32 [7168], replicated, may hold values from 0.25 to 1.75
- final_gain: float32 [7168], replicated, may hold values from 0.25 to 1.75
- pool_weights: bfloat16 [2, 16, 6144, 7168], P('pool', 'dev'), may hold values from -0.28347335 to 0.28347335
- expert_ids: int32 [256, 4], P('dev'), may hold values from 0 to 15, all different within a row; in each aligned block of 16 rows (0 to 15, 16 to 31, ...) at most 8 rows name the same one
- gate_weights: float32 [256, 4], P('dev'), may hold values from 0.05 to 0.6
- draft_ids: int32 [256], replicated, may hold values from 0 to 98303
Outputs:
- draft_logprob: float32 [256], replicated
The draws below stay inside these ranges and needn't reach their ends.
Inputs may be any that keep to these rules, and one draw needn't show every extreme that they name: `expert_ids`: each row names 4 different experts. Within one owner's rows (aligned blocks of 16 rows) no expert is named by more than 8 rows; in some owners' rows an expert is named by exactly 8.
All inputs are finite; a program needn't handle non-finite values.
Results may differ from the reference program's by a relative error of at most 0.0008.
Values may be sent and summed in bfloat16 or wider, within the bound.
A program may use at most 192 MiB of HBM per device.

```python
import math
import jax
import jax.numpy as jnp
import numpy as np
from jax import lax

D = 7168
FF = 2048
EXPERTS = 16
TOP = 4
TOK_OWN = 16
TOKENS = 256
CAP = 8
GROUP = 1
FF_DEV = 2048
ROWS_DEV = 6144
VOCAB = 98304
N_DEV = 16


aligned_count = 8


pair_count = 4


def shared_picks(key):
    picks_key = jax.random.fold_in(key, 7001)
    directions = jnp.clip(jax.random.normal(jax.random.fold_in(picks_key, 1), (aligned_count, D), jnp.float32), -4.0, 4.0)
    vocab_rows = jax.random.permutation(jax.random.fold_in(picks_key, 2), VOCAB)[:aligned_count].astype(jnp.int32)
    token_rows = jax.random.permutation(jax.random.fold_in(picks_key, 3), TOKENS)[:pair_count].astype(jnp.int32)
    strengths = jax.random.uniform(jax.random.fold_in(picks_key, 4), (pair_count,), jnp.float32, 1.0, 2.0)
    partner = jax.random.uniform(jax.random.fold_in(picks_key, 5), (pair_count, 1), jnp.float32, 0.988, 0.994)
    return (directions, vocab_rows, token_rows, strengths, partner)


def draw_pool_weights(key, part):
    directions, vocab_rows, token_rows, strengths, partner = shared_picks(key)
    vocab_scale = 4.0 / math.sqrt(D)
    aligned_rows = directions * (210.0 / D * jnp.repeat(strengths, 2))[:, None]
    expert_scales = jnp.array([1.0 / math.sqrt(D), 1.0 / math.sqrt(D), 1.0 / math.sqrt(FF)], jnp.float32)
    row_ids = jnp.arange(ROWS_DEV, dtype=jnp.int32)
    row_scales = expert_scales[row_ids // FF_DEV]

    def one_shard(shard_index):
        vocab_block = jnp.clip(jax.random.normal(jax.random.fold_in(jax.random.fold_in(key, 31), shard_index), (ROWS_DEV, D), jnp.float32), -6.0, 6.0) * vocab_scale
        match_rows = ((shard_index * ROWS_DEV + row_ids)[:, None] == vocab_rows[None, :]).astype(jnp.float32)
        vocab_block = vocab_block * (1.0 - jnp.sum(match_rows, axis=1, keepdims=True)) + jnp.dot(match_rows, aligned_rows, precision=lax.Precision.HIGHEST)
        expert_rows = jnp.clip(jax.random.normal(jax.random.fold_in(jax.random.fold_in(key, 32), shard_index), (ROWS_DEV, D), jnp.float32), -6.0, 6.0)
        return (vocab_block.astype(jnp.bfloat16), (expert_rows * row_scales[:, None]).astype(jnp.bfloat16))
    vocab_all, expert_all = lax.map(one_shard, jnp.arange(N_DEV, dtype=jnp.int32))
    return jnp.stack([expert_all, vocab_all])


def draw_hidden(key, part):
    gaussian = jnp.clip(jax.random.normal(jax.random.fold_in(key, 41), (TOKENS, D), jnp.float32), -4.0, 4.0)
    values = gaussian
    directions, vocab_rows, token_rows, strengths, partner = shared_picks(key)
    size_factor = jax.random.uniform(jax.random.fold_in(key, 45), (pair_count, 1), jnp.float32, 4.0, 7.0)
    aligned = size_factor * (directions[0::2] + partner * directions[1::2])
    values = values.at[token_rows].set(aligned)
    return values.astype(jnp.bfloat16)


def place_ends(entries, stream_key, least, top_value):
    longest = entries.shape.index(max(entries.shape))
    spots = []
    for shift in (0, 1):
        where = [jax.random.randint(jax.random.fold_in(stream_key, axis), (), 0, length) for axis, length in enumerate(entries.shape)]
        where[longest] = (where[longest] + shift) % entries.shape[longest]
        spots.append(tuple(where))
    return entries.at[spots[0]].set(least).at[spots[1]].set(top_value)


def shard_levels(key, extent, split, least, high):
    loudness = 1.0
    for axis_at, shards_of in split:
        draws = jax.random.uniform(jax.random.fold_in(jax.random.fold_in(key, 6), axis_at), (shards_of,), jnp.float32, least / len(split), high / len(split))
        loudness = loudness * jnp.repeat(jnp.exp(draws), extent[axis_at] // shards_of).reshape((-1,) + (1,) * (len(extent) - 1 - axis_at))
    return loudness


def ranked_wide(own_key, shape, count, slope):
    loads = [min(1 << octave, count + 1 - (1 << octave)) * (1 << 20) // math.isqrt((1 << octave) ** slope) + 1 for octave in range((count + 1).bit_length()) if 1 << octave <= count]
    scale = 1 + sum(loads) // (1 << 30)
    grid = np.cumsum(np.array([max(1, weight // scale) for weight in loads]))
    lot = jax.random.randint(jax.random.fold_in(own_key, 1), shape, 0, int(grid[len(loads) - 1]))
    start = jnp.left_shift(1, jnp.searchsorted(jnp.asarray(grid, jnp.int32), lot, side="right").astype(jnp.int32))
    standing = start - 1 + jax.random.randint(jax.random.fold_in(own_key, 4), shape, 0, 1 << 30) % jnp.minimum(start, count + 1 - start)
    return jax.random.permutation(jax.random.fold_in(own_key, 2), count)[standing].astype(jnp.int32)


def assign_block(key, own, number, rows, amount, top, reach, slope):
    ranking = jax.random.permutation(key, amount)
    packed, usual = load_shares(amount, rows * top, reach, slope, True), load_shares(amount, rows * top, reach, slope, False)
    places = jnp.arange(amount)

    def named(tallies, turn):
        used = int((tallies > 0).sum())
        fixed = max(1, used // 4)
        passed = fixed + (places - fixed + turn * (used - fixed)) % max(1, amount - fixed)
        return jnp.zeros((amount,), jnp.int32).at[ranking[jnp.where(places < fixed, places, passed)]].set(jnp.asarray(tallies, jnp.int32))

    tallies = jnp.where(number % 4 == 0, named(packed, number // 4), named(usual, number - number // 4 - 1))
    mixed = jax.random.permutation(jax.random.fold_in(own, 3), amount)
    giver, receiver = mixed[0:amount // 2 * 2:2], mixed[1:amount // 2 * 2:2]
    room = jnp.minimum(tallies[giver] - 1, reach - tallies[receiver]) // 2
    room = jnp.where((giver == ranking[0]) | (receiver == ranking[0]) | (tallies[receiver] == 0), 0, jnp.maximum(room, 0))
    passed = jax.random.randint(jax.random.fold_in(own, 4), (amount // 2,), 0, 1 << 20) % (room + 1)
    tallies = tallies.at[giver].add(-passed).at[receiver].add(passed)
    members = jnp.searchsorted(jnp.cumsum(tallies), jnp.arange(rows * top), side="right").astype(jnp.int32)
    listing = members.reshape(top, rows).T
    listing = listing[jax.random.permutation(jax.random.fold_in(own, 1), rows)]
    turn = jax.random.randint(jax.random.fold_in(own, 2), (rows, 1), 0, top)
    return jnp.take_along_axis(listing, (jnp.arange(top)[None, :] + turn) % top, axis=1)


def load_shares(amount, total, limit, lean, full):
    weights = [(1 << 20) // math.isqrt(standing ** lean) + 1 for standing in range(1, amount + 1)]
    largest = limit if full else min(limit, max(-(-total // amount), total * weights[0] // sum(weights)))
    least = 1 if total - largest >= amount - 1 else 0
    given, surplus = [largest] + [least] * (amount - 1), total - largest - least * (amount - 1)
    while surplus > 0:
        movable = [i for i in range(1, amount) if given[i] < largest] or [i for i in range(1, amount) if given[i] < limit]
        whole, left = sum([weights[i] for i in movable]), surplus
        for i in movable:
            addition = min(limit - given[i], max(1, left * weights[i] // whole), surplus)
            given[i] = given[i] + addition
            surplus = surplus - addition
    return np.array(given)


def setup_inputs(seed: int = 0) -> dict:
    streams_of = jax.random.split(jax.random.key(seed), 8)
    hidden = draw_hidden(jax.random.fold_in(streams_of[7], 71), 0)
    ffn_gain = jnp.clip(1.0 + 0.15 * jax.random.normal(streams_of[1], (D,), jnp.float32), 0.25, 1.75)
    final_gain = jnp.clip(1.0 + 0.15 * jax.random.normal(streams_of[2], (D,), jnp.float32), 0.25, 1.75)
    pool_weights = draw_pool_weights(jax.random.fold_in(streams_of[7], 71), 0)
    expert_ids_keys = jax.random.split(jax.random.fold_in(streams_of[4], 1), TOKENS // TOK_OWN)
    expert_ids_turns = jax.random.permutation(jax.random.fold_in(streams_of[4], 3), TOKENS // TOK_OWN)
    expert_ids = jax.vmap(lambda own, number: assign_block(jax.random.fold_in(streams_of[4], 2), own, number, TOK_OWN, EXPERTS, TOP, CAP, 2))(expert_ids_keys, expert_ids_turns).reshape((TOKENS, TOP))
    gate_weights = jnp.clip(0.05 + 0.55 * jax.random.uniform(streams_of[5], (TOKENS, TOP), jnp.float32) ** shard_levels(streams_of[5], (TOKENS, TOP), ((0, 16),), -0.2, 0.2), 0.05, 0.6)
    draft_ids = place_ends(ranked_wide(streams_of[6], (TOKENS,), VOCAB, 2), jax.random.fold_in(streams_of[6], 3), 0, VOCAB - 1).astype(jnp.int32)
    return dict(hidden=hidden, ffn_gain=ffn_gain, final_gain=final_gain, pool_weights=pool_weights, expert_ids=expert_ids, gate_weights=gate_weights, draft_ids=draft_ids)


norm_eps = 1e-06

def rms_norm(values_in, scale_gain):
    mean_square = lax.optimization_barrier(jnp.mean(values_in * values_in, axis=-1, keepdims=True))
    return values_in * lax.rsqrt(mean_square + norm_eps) * scale_gain

def reference(hidden, ffn_gain, final_gain, pool_weights, expert_ids, gate_weights, draft_ids):
    residual = hidden.astype(jnp.float32)
    normed = rms_norm(residual, ffn_gain).astype(jnp.bfloat16)
    owner_ids = expert_ids.reshape(N_DEV, TOK_OWN * TOP)
    onehot = (owner_ids[:, :, None] == jnp.arange(EXPERTS, dtype=jnp.int32)[None, None, :]).astype(jnp.int32)
    slot_rank = lax.optimization_barrier(jnp.sum((jnp.cumsum(onehot, axis=1) - onehot) * onehot, axis=2))
    owners = jnp.arange(N_DEV, dtype=jnp.int32)[:, None]
    flat_index = ((owner_ids * N_DEV + owners) * CAP + slot_rank).reshape(TOKENS * TOP).astype(jnp.int32)
    token_index = jnp.repeat(jnp.arange(TOKENS, dtype=jnp.int32), TOP)
    buffer = jnp.zeros((EXPERTS * N_DEV * CAP, D), jnp.bfloat16).at[flat_index].set(normed[token_index])
    expert_weights = pool_weights[0].reshape(EXPERTS, GROUP, 3, FF_DEV, D)

    def run_expert(inputs):
        row_block, weight_block = inputs
        accumulated = jnp.zeros((N_DEV * CAP, D), jnp.float32)
        for member in range(GROUP):
            gate_proj = jnp.dot(row_block, weight_block[member, 0].T, preferred_element_type=jnp.float32)
            up_proj = jnp.dot(row_block, weight_block[member, 1].T, preferred_element_type=jnp.float32)
            activated = (jax.nn.silu(gate_proj) * up_proj).astype(jnp.bfloat16)
            member_part = jnp.dot(activated, weight_block[member, 2], preferred_element_type=jnp.float32).astype(jnp.bfloat16)
            accumulated = accumulated + member_part.astype(jnp.float32)
        return accumulated
    outputs = lax.map(run_expert, (buffer.reshape(EXPERTS, N_DEV * CAP, D), expert_weights))
    outputs = outputs.reshape(EXPERTS * N_DEV * CAP, D)
    picked = jnp.take(outputs, flat_index, axis=0).reshape(TOKENS, TOP, D)
    mixture = lax.optimization_barrier(jnp.sum(picked * gate_weights[:, :, None], axis=1))
    normed_final = rms_norm(residual + mixture, final_gain).astype(jnp.bfloat16)
    columns = jnp.arange(ROWS_DEV, dtype=jnp.int32)

    def shard_stats(inputs):
        vocab_block, first_column = inputs
        shard_logit = jnp.dot(normed_final, vocab_block.T, preferred_element_type=jnp.float32)
        peak_logit = lax.optimization_barrier(jnp.max(shard_logit, axis=1))
        exp_total = lax.optimization_barrier(jnp.sum(jnp.exp(shard_logit - peak_logit[:, None]), axis=1))
        target = lax.optimization_barrier(jnp.sum(jnp.where(columns[None, :] == (draft_ids - first_column)[:, None], shard_logit, 0.0), axis=1))
        return (peak_logit, exp_total, target)
    firsts = (jnp.arange(N_DEV, dtype=jnp.int32) * ROWS_DEV).astype(jnp.int32)
    peaks, totals, targets = lax.map(shard_stats, (pool_weights[1], firsts))
    row_max = lax.optimization_barrier(jnp.max(peaks, axis=0))
    exp_total = lax.optimization_barrier(jnp.sum(totals * jnp.exp(peaks - row_max[None, :]), axis=0))
    return lax.optimization_barrier(jnp.sum(targets, axis=0)) - row_max - jnp.log(exp_total)
```

```python
import functools

import jax
import jax.numpy as jnp
from jax import lax
from jax.experimental import pallas as pl
from jax.experimental.pallas import tpu as pltpu
from jax.sharding import PartitionSpec as P

EXPERTS = 16
LANES = 128
COLS = 512
LINE = 4
MESH = pl.DeviceIdType.MESH

norm_eps = 1e-06
neg_fill = -1e30


def rms_norm(values_in, scale_gain):
    mean_square = jnp.mean(values_in * values_in, axis=-1, keepdims=True)
    return values_in * lax.rsqrt(mean_square + norm_eps) * scale_gain


def kernel(
    n, slots, hidden_ref, ffn_gain_ref, final_gain_ref, placing_ref, mixing_ref, draft_ref, w_hbm,
    out_ref,
    w_buf, packed, landed, part, x_buf, act, final_buf, stat_out, stat_all, result,
    tops, sums, picks,
    w_sem, s1_send, s1_recv, s2_send, s2_recv, ag_send, ag_recv, st_send, st_recv, res_send, res_recv,
):
    pool = lax.axis_index("pool")
    me = lax.axis_index("dev")
    group = n // EXPERTS
    tile = w_buf.shape[1]
    rows_dev, width = w_hbm.shape
    tiles = rows_dev // tile
    ff_tiles = tiles // 3
    capacity = packed.shape[1]
    tok_own = hidden_ref.shape[0]
    flat = n * capacity

    def fetch(row_tile, slot):
        start = pl.multiple_of(row_tile * tile, tile)
        return pltpu.make_async_copy(w_hbm.at[pl.ds(start, tile)], w_buf.at[slot], w_sem.at[slot])

    def send(src, dst, send_sem, recv_sem, to_pool, to_dev):
        return pltpu.make_async_remote_copy(
            src_ref=src, dst_ref=dst, send_sem=send_sem, recv_sem=recv_sem,
            device_id=(to_pool, to_dev), device_id_type=MESH,
        )

    def expert_order(t):
        return jnp.where(t < 2 * ff_tiles, (t % 2) * ff_tiles + t // 2, t)

    @pl.when(pool == 0)
    def _():
        normed = rms_norm(hidden_ref[...].astype(jnp.float32), ffn_gain_ref[...]).astype(jnp.bfloat16)
        rows = jnp.dot(placing_ref[...], normed, preferred_element_type=jnp.float32)
        packed[...] = rows.reshape(packed.shape).astype(jnp.bfloat16)
        out_copies = []
        for k in range(1, n):
            to = lax.rem(me + k, n)
            c = send(packed.at[to // group], landed.at[me], s1_send.at[k], s1_recv.at[me], 0, to)
            c.start()
            out_copies.append(c)
        for t in range(slots):
            fetch(expert_order(jnp.int32(t)), t).start()
        landed[me] = packed[me // group]
        for k in range(1, n):
            src = lax.rem(me + n - k, n)
            send(packed.at[0], landed.at[src], s1_send.at[k], s1_recv.at[src], 0, src).wait_recv()
        for c in out_copies:
            c.wait_send()

        def unpack(c, _):
            cols = pl.ds(pl.multiple_of(c * COLS, COLS), COLS)
            x_buf[:flat, cols] = (
                landed[:, :, cols].astype(jnp.float32).reshape(flat, COLS).astype(jnp.bfloat16)
            )
            return 0

        lax.fori_loop(0, width // COLS, unpack, 0)

        def gate_up(j, _):
            halves = []
            for h in range(2):
                t = 2 * j + h
                slot = lax.rem(t, slots)
                fetch(0, slot).wait()
                halves.append(
                    lax.dot_general(
                        x_buf[:flat], w_buf[slot], (((1,), (1,)), ((), ())),
                        preferred_element_type=jnp.float32,
                    )
                )

                @pl.when(t + slots < tiles)
                def _():
                    fetch(expert_order(t + slots), slot).start()

            gate, up = halves
            act[j] = (gate / (1.0 + jnp.exp(-gate)) * up).astype(jnp.bfloat16)
            return 0

        lax.fori_loop(0, ff_tiles, gate_up, 0)
        for t in range(2 * ff_tiles, tiles):
            fetch(0, t % slots).wait()

        def down(c, _):
            cols = pl.ds(pl.multiple_of(c * COLS, COLS), COLS)
            total = jnp.zeros((flat, COLS), jnp.float32)
            for i in range(ff_tiles):
                total += jnp.dot(
                    act[i], w_buf[(2 * ff_tiles + i) % slots, :, cols],
                    preferred_element_type=jnp.float32,
                )
            part[:, :, cols] = total.reshape(n, capacity, COLS).astype(jnp.bfloat16)
            return 0

        lax.fori_loop(0, width // COLS, down, 0)
        back = []
        for k in range(n):
            to = lax.rem(me + k, n)
            c = send(part.at[to], landed.at[me], s2_send.at[k], s2_recv.at[me], 1, to)
            c.start()
            back.append(c)
        for c in back:
            c.wait_send()
        send(result, result, res_send, res_recv, 1, me).wait_recv()

    @pl.when(pool == 1)
    def _():
        for t in range(slots):
            fetch(t, t).start()
        for k in range(n):
            src = lax.rem(me + n - k, n)
            send(part.at[0], landed.at[src], s2_send.at[k], s2_recv.at[src], 0, src).wait_recv()
        mix = mixing_ref[...]
        high = mix.astype(jnp.bfloat16)
        rest = mix - high.astype(jnp.float32)
        mid = rest.astype(jnp.bfloat16)
        low = (rest - mid.astype(jnp.float32)).astype(jnp.bfloat16)

        def combine(c, square):
            cols = pl.ds(pl.multiple_of(c * COLS, COLS), COLS)
            rows = landed[:, :, cols].astype(jnp.float32).reshape(flat, COLS).astype(jnp.bfloat16)
            moe = jnp.dot(high, rows, preferred_element_type=jnp.float32)
            moe += jnp.dot(mid, rows, preferred_element_type=jnp.float32)
            moe += jnp.dot(low, rows, preferred_element_type=jnp.float32)
            final = hidden_ref[:, cols].astype(jnp.float32) + moe
            final_buf[:, cols] = final
            return square + jnp.sum(final * final, axis=1, keepdims=True)

        square = lax.fori_loop(0, width // COLS, combine, jnp.zeros((tok_own, 1), jnp.float32))
        scale = lax.rsqrt(square / width + norm_eps)
        mine = pl.ds(pl.multiple_of(me * tok_own, tok_own), tok_own)
        x_buf[mine] = (final_buf[...] * scale * final_gain_ref[...]).astype(jnp.bfloat16)

        lines = n // LINE
        hi, lo = me // LINE, lax.rem(me, LINE)

        def rows_of(dev):
            return pl.ds(pl.multiple_of(dev * tok_own, tok_own), tok_own)

        sent = []
        count = 0

        def push(owner, to):
            nonlocal count
            c = send(
                x_buf.at[rows_of(owner)], x_buf.at[rows_of(owner)],
                ag_send.at[count], ag_recv.at[owner], 1, to,
            )
            c.start()
            count += 1
            sent.append(c)

        def arrive(owner):
            send(
                x_buf.at[rows_of(owner)], x_buf.at[rows_of(owner)],
                ag_send.at[0], ag_recv.at[owner], 1, owner,
            ).wait_recv()

        for h in range(1, lines):
            push(me, lax.rem(hi + h, lines) * LINE + lo)
        for h in range(lines):
            owner = lax.rem(hi + lines - h, lines) * LINE + lo
            if h:
                arrive(owner)
            for l in range(1, LINE):
                push(owner, hi * LINE + lax.rem(lo + l, LINE))
        for h in range(lines):
            for l in range(1, LINE):
                arrive(lax.rem(hi + lines - h, lines) * LINE + lax.rem(lo + LINE - l, LINE))
        for c in sent:
            c.wait_send()

        tops[...] = jnp.full_like(tops, neg_fill)
        sums[...] = jnp.zeros_like(sums)
        picks[...] = jnp.zeros_like(picks)

        def score(t, _):
            slot = lax.rem(t, slots)
            fetch(0, slot).wait()
            logits = lax.dot_general(
                x_buf[...], w_buf[slot], (((1,), (1,)), ((), ())),
                preferred_element_type=jnp.float32,
            )

            @pl.when(t + slots < tiles)
            def _():
                fetch(t + slots, slot).start()

            target = draft_ref[...] - (me * rows_dev + t * tile)
            lane = lax.broadcasted_iota(jnp.int32, (logits.shape[0], LANES), 1)
            pieces = [logits[:, i * LANES : (i + 1) * LANES] for i in range(tile // LANES)]
            old = tops[...]
            top = functools.reduce(jnp.maximum, pieces, old)
            total = sums[...] * jnp.exp(old - top)
            pick = picks[...]
            for i, piece in enumerate(pieces):
                total += jnp.exp(piece - top)
                pick += jnp.where(lane + i * LANES == target, piece, 0.0)
            tops[...] = top
            sums[...] = total
            picks[...] = pick
            return 0

        lax.fori_loop(0, tiles, score, 0)
        tall = tops[...].T
        top = jnp.max(tall, axis=0, keepdims=True)
        total = jnp.sum(sums[...].T * jnp.exp(tall - top), axis=0, keepdims=True)
        pick = jnp.sum(picks[...].T, axis=0, keepdims=True)
        mine_stats = jnp.concatenate([top, total, pick, jnp.zeros((5, top.shape[1]), jnp.float32)], axis=0)
        stat_out[...] = mine_stats
        told = []
        for k in range(1, n):
            to = lax.rem(me + k, n)
            c = send(stat_out, stat_all.at[me], st_send.at[k], st_recv.at[me], 1, to)
            c.start()
            told.append(c)
        stat_all[me] = mine_stats
        for k in range(1, n):
            src = lax.rem(me + n - k, n)
            send(stat_out, stat_all.at[src], st_send.at[k], st_recv.at[src], 1, src).wait_recv()
        every = stat_all[...]
        best = jnp.max(every[:, 0:1, :], axis=0)
        exp_total = jnp.sum(every[:, 1:2, :] * jnp.exp(every[:, 0:1, :] - best[None]), axis=0)
        drafted = jnp.sum(every[:, 2:3, :], axis=0)
        result[...] = jnp.broadcast_to(drafted - best - jnp.log(exp_total), result.shape)
        c = send(result, result, res_send, res_recv, 0, me)
        c.start()
        for d in told:
            d.wait_send()
        c.wait_send()

    out_ref[...] = result[...]


def shards(hidden, ffn_gain, final_gain, pool_weights, expert_ids, gate_weights, draft_ids):
    n = lax.axis_size("dev")
    group = n // EXPERTS
    tok_own, width = hidden.shape
    capacity = tok_own // 2
    tokens = draft_ids.shape[0]
    weights = pool_weights[0, 0]
    rows_dev = weights.shape[0]
    tile = 512 if n <= 16 else 256
    slots = min(6 if n <= 16 else 4, rows_dev // tile)
    top_count = expert_ids.shape[1]
    places = EXPERTS * capacity

    onehot = (expert_ids[:, :, None] == jnp.arange(EXPERTS, dtype=jnp.int32)).astype(jnp.int32)
    named = jnp.sum(onehot, axis=1)
    earlier = jnp.arange(tok_own)[:, None] > jnp.arange(tok_own)[None, :]
    before = jnp.sum(jnp.where(earlier[:, :, None], named[None], 0), axis=1)
    rank = jnp.sum(onehot * before[:, None, :], axis=2)
    flat_slot = expert_ids * capacity + rank
    hits = flat_slot[:, :, None] == jnp.arange(places, dtype=jnp.int32)
    placing = jnp.any(hits, axis=1).astype(jnp.bfloat16).T
    mixing = jnp.sum(jnp.where(hits, gate_weights[:, :, None], 0.0), axis=1)
    mixing = jnp.broadcast_to(
        mixing.reshape(tok_own, EXPERTS, 1, capacity), (tok_own, EXPERTS, group, capacity)
    ).reshape(tok_own, n * capacity)

    vmem = pl.BlockSpec(memory_space=pltpu.VMEM)
    dma = pltpu.SemaphoreType.DMA
    lines = n // LINE
    out = pl.pallas_call(
        functools.partial(kernel, n, slots),
        out_shape=jax.ShapeDtypeStruct((8, tokens), jnp.float32),
        in_specs=[vmem] * 6 + [pl.BlockSpec(memory_space=pl.ANY)],
        out_specs=vmem,
        scratch_shapes=[
            pltpu.VMEM((slots, tile, width), jnp.bfloat16),
            pltpu.VMEM((EXPERTS, capacity, width), jnp.bfloat16),
            pltpu.VMEM((n, capacity, width), jnp.bfloat16),
            pltpu.VMEM((n, capacity, width), jnp.bfloat16),
            pltpu.VMEM((tokens, width), jnp.bfloat16),
            pltpu.VMEM((rows_dev // 3 // tile, n * capacity, tile), jnp.bfloat16),
            pltpu.VMEM((tok_own, width), jnp.float32),
            pltpu.VMEM((8, tokens), jnp.float32),
            pltpu.VMEM((n, 8, tokens), jnp.float32),
            pltpu.VMEM((8, tokens), jnp.float32),
            pltpu.VMEM((tokens, LANES), jnp.float32),
            pltpu.VMEM((tokens, LANES), jnp.float32),
            pltpu.VMEM((tokens, LANES), jnp.float32),
            dma((slots,)),
            dma((n,)), dma((n,)), dma((n,)), dma((n,)),
            dma((n + lines,)), dma((n,)),
            dma((n,)), dma((n,)), dma, dma,
        ],
        compiler_params=pltpu.CompilerParams(has_side_effects=True, vmem_limit_bytes=66_000_000),
    )(
        hidden, ffn_gain[None], final_gain[None], placing, mixing, draft_ids[:, None], weights,
    )
    return out[0]


def solution(mesh):
    return jax.shard_map(
        shards,
        mesh=mesh,
        in_specs=(
            P("dev", None),
            P(),
            P(),
            P("pool", "dev", None, None),
            P("dev", None),
            P("dev", None),
            P(),
        ),
        out_specs=P(),
        check_vma=False,
    )
```
